256 devices in a mesh: gx: 8 (over z), gy: 8 (over y_lo, x), gz: 4 (over y_hi, core).
Axes of the slice: x: 4, y: 4 (y_hi: 2, y_lo: 2; y = y_hi * 2 + y_lo), z: 8, core: 2. Of those that a mesh axis runs over, the one named last changes fastest.
Arguments:
- constraint: bfloat16 [8, 8, 4, 256, 3072], P('gx', 'gy', 'gz'), may hold values from -1.5 to 1.5
- stiff_ib: bfloat16 [8, 8, 4, 256, 3072], P('gx', 'gy', 'gz'), may hold values from -0.75 to 0.75
- mass_ib: bfloat16 [8, 8, 4, 256, 3072], P('gx', 'gy', 'gz'), may hold values from -1.5 to 1.5
- mass_ii: float32 [8, 8, 4, 256], P('gx', 'gy', 'gz'), may hold values from 0.5 to 4
- modes: bfloat16 [8, 8, 4, 300, 256], P('gx', 'gy', 'gz'), may hold values from -0.375 to 0.375
- stiff_faces: bfloat16 [8, 8, 4, 6, 512, 512], P('gx', 'gy', 'gz'), may hold values from -3 to 3
- mass_faces: bfloat16 [8, 8, 4, 6, 512], P('gx', 'gy', 'gz'), may hold values from 0.19921875 to 4
- dof_map: int32 [8, 8, 4, 3, 512], P('gx', 'gy', 'gz'), may hold values from 0 to 511, each once within a row
Outputs:
- stiff_assembled: bfloat16 [8, 8, 4, 3, 512, 512], P('gx', 'gy', 'gz')
- mass_assembled: bfloat16 [8, 8, 4, 3, 512, 512], P('gx', 'gy', 'gz')
- modal_coupling: bfloat16 [8, 8, 4, 3, 600, 512], P('gx', 'gy', 'gz')
The draws below stay inside these ranges and needn't reach their ends.
Inputs may be any that keep to these rules, and one draw needn't show every extreme that they name: `dof_map`: each row of the last dimension is a permutation of 0 to 511.
All inputs are finite; a program needn't handle non-finite values.
Results may differ from the reference program's by a relative error of at most 0.0075.
Values may be sent and summed in bfloat16 or wider, within the bound.
A program may use at most 64 MiB of HBM per device.

```python
import math
import jax
import jax.numpy as jnp
from jax import lax

FACE = 512
MODES = 300
NI = 256
B = 3072
N_GX = 8
N_GY = 8
N_GZ = 4


def block_levels(key, dims, split, smallest, top_value):
    def one(axis_at, shards_of):
        heights = jax.random.uniform(jax.random.fold_in(jax.random.fold_in(key, 6), axis_at), (shards_of,), jnp.float32, smallest / len(split), top_value / len(split))
        return jnp.repeat(jnp.exp(heights), dims[axis_at] // shards_of).reshape((-1,) + (1,) * (len(dims) - axis_at - 1))

    level = one(*split[0])
    for cut in split[1:]:
        level = level * one(*cut)
    return level


def centred(key, dims, scale, bound, shards=(), held_as=jnp.bfloat16):
    array = scale * jax.random.normal(key, dims, jnp.float32)
    if shards:
        array = array * block_levels(key, dims, shards, -0.22, 0.18)
    return jnp.clip(array, -bound, bound).astype(held_as)


def setup_inputs(seed: int = 0) -> dict:
    key_of = jax.random.split(jax.random.key(seed), 9)
    constraint = centred(key_of[0], (N_GX, N_GY, N_GZ, NI, B), 0.25, 1.5, ((0, 8), (1, 8), (2, 4)))
    stiff_ib = centred(key_of[1], (N_GX, N_GY, N_GZ, NI, B), (NI // 4) ** -0.5, 0.75, ((0, 8), (1, 8), (2, 4)))
    mass_ib = centred(key_of[2], (N_GX, N_GY, N_GZ, NI, B), 0.25, 1.5, ((0, 8), (1, 8), (2, 4)))
    mass_ii = jnp.clip(jnp.exp(math.log(4.0) - 2.0794415 * jax.random.uniform(key_of[3], (N_GX, N_GY, N_GZ, NI), jnp.float32) ** block_levels(key_of[3], (N_GX, N_GY, N_GZ, NI), ((0, 8), (1, 8), (2, 4)), -0.2, 0.2)), 0.5, 4.0)
    modes = centred(key_of[4], (N_GX, N_GY, N_GZ, MODES, NI), NI ** -0.5, 0.375, ((0, 8), (1, 8), (2, 4)))
    stiff_faces = centred(key_of[5], (N_GX, N_GY, N_GZ, 6, FACE, FACE), 0.5, 3.0, ((0, 8), (1, 8), (2, 4)))
    mass_faces = jnp.clip(jnp.exp(math.log(4.0) - 2.9996462 * jax.random.uniform(key_of[6], (N_GX, N_GY, N_GZ, 6, FACE), jnp.float32) ** block_levels(key_of[6], (N_GX, N_GY, N_GZ, 6, FACE), ((0, 8), (1, 8), (2, 4)), -0.2, 0.2)), 0.19921875, 4.0).astype(jnp.bfloat16)
    dof_map = jax.vmap(lambda own: jax.random.permutation(own, FACE))(jax.random.split(key_of[7], N_GX * N_GY * N_GZ * 3)).reshape((N_GX, N_GY, N_GZ, 3, FACE)).astype(jnp.int32)
    return dict(constraint=constraint, stiff_ib=stiff_ib, mass_ib=mass_ib, mass_ii=mass_ii, modes=modes, stiff_faces=stiff_faces, mass_faces=mass_faces, dof_map=dof_map)


def transposed(left, right):
    return lax.dot_general(left, right, (((0,), (0,)), ((), ())), preferred_element_type=jnp.float32)


def superelement(items):
    constraint, stiff_ib, mass_ib, mass_ii, modes, stiff_faces, mass_faces = items
    loaded = (mass_ib.astype(jnp.float32) + mass_ii[:, None] * constraint.astype(jnp.float32)).astype(jnp.bfloat16)
    coupling = jnp.dot(modes, loaded, preferred_element_type=jnp.float32).astype(jnp.bfloat16)
    width = stiff_faces.shape[-1]
    stiff_list = []
    mass_list = []
    for face in range(6):
        lower = face * width
        stiff_cols = stiff_ib[:, lower:lower + width]
        mass_cols = mass_ib[:, lower:lower + width]
        cons_cols = constraint[:, lower:lower + width]
        load_cols = loaded[:, lower:lower + width]
        stiff_list.append((stiff_faces[face].astype(jnp.float32) + transposed(stiff_cols, cons_cols)).astype(jnp.bfloat16))
        mass_list.append((jnp.diag(mass_faces[face].astype(jnp.float32)) + transposed(cons_cols, load_cols) + transposed(mass_cols, cons_cols)).astype(jnp.bfloat16))
    return jnp.stack(stiff_list), jnp.stack(mass_list), coupling


def upper_neighbour(values, axis):
    size = values.shape[axis]
    rest = lax.slice_in_dim(values, 1, size, axis=axis)
    pad = jnp.zeros_like(lax.slice_in_dim(values, 0, 1, axis=axis))
    return jnp.concatenate([rest, pad], axis=axis)


def reference(constraint, stiff_ib, mass_ib, mass_ii, modes, stiff_faces, mass_faces, dof_map):
    grid = constraint.shape[:3]
    count = grid[0] * grid[1] * grid[2]
    items = tuple(a.reshape((count,) + a.shape[3:]) for a in (constraint, stiff_ib, mass_ib, mass_ii, modes, stiff_faces, mass_faces))
    stiff_red, mass_red, coupling = lax.map(superelement, items)
    stiff_red = stiff_red.reshape(grid + stiff_red.shape[1:])
    mass_red = mass_red.reshape(grid + mass_red.shape[1:])
    coupling = coupling.reshape(grid + coupling.shape[1:])
    width = stiff_red.shape[-1]
    stiff_out = []
    mass_out = []
    coup_out = []
    for axis in range(3):
        mapping = dof_map[:, :, :, axis, :].astype(jnp.int32)
        high = 2 * axis + 1
        low = 2 * axis
        stiff_nb = upper_neighbour(stiff_red[:, :, :, low], axis)
        mass_nb = upper_neighbour(mass_red[:, :, :, low], axis)
        coup_nb = upper_neighbour(coupling[:, :, :, :, low * width:(low + 1) * width], axis)
        rows = mapping[:, :, :, :, None]
        cols = mapping[:, :, :, None, :]
        stiff_nb = jnp.take_along_axis(jnp.take_along_axis(stiff_nb, rows, axis=3), cols, axis=4)
        mass_nb = jnp.take_along_axis(jnp.take_along_axis(mass_nb, rows, axis=3), cols, axis=4)
        coup_nb = jnp.take_along_axis(coup_nb, cols, axis=4)
        stiff_out.append((stiff_red[:, :, :, high].astype(jnp.float32) + stiff_nb.astype(jnp.float32)).astype(jnp.bfloat16))
        mass_out.append((mass_red[:, :, :, high].astype(jnp.float32) + mass_nb.astype(jnp.float32)).astype(jnp.bfloat16))
        coup_out.append(jnp.concatenate([coupling[:, :, :, :, high * width:(high + 1) * width], coup_nb], axis=3))
    return jnp.stack(stiff_out, axis=3), jnp.stack(mass_out, axis=3), jnp.stack(coup_out, axis=3)
```

```python
import functools

import jax
import jax.numpy as jnp
from jax import lax
from jax.experimental import pallas as pl
from jax.experimental.pallas import tpu as pltpu
from jax.sharding import PartitionSpec as P

MESH = pl.DeviceIdType.MESH
AXES = ("gx", "gy", "gz")
BF16 = jnp.bfloat16
F32 = jnp.float32


def turned(left, right):
    return lax.dot_general(left, right, (((0,), (0,)), ((), ())), preferred_element_type=F32)


def times(left, right):
    return jnp.dot(left, right, preferred_element_type=F32)


def column_of(row, lanes=128):
    return jnp.broadcast_to(row, (lanes, row.shape[1])).T


def exchange(
    sizes,
    parts,
    cons_in,
    stiff_in,
    mass_in,
    mii_in,
    modes_in,
    faces_in,
    mfaces_in,
    dof_in,
    stiff_out,
    mass_out,
    coup_out,
    cons,
    stiff,
    mass,
    mii,
    modes,
    faces,
    mfaces,
    dof,
    lump,
    load,
    select,
    select_t,
    dcol,
    full,
    half,
    stiff_send,
    mass_send,
    diag_send,
    coup_send,
    stiff_recv,
    mass_recv,
    diag_recv,
    coup_recv,
    col_sem,
    face_sem,
    small_sem,
    stiff_sems,
    mass_sems,
    diag_sems,
    coup_sems,
):
    width = faces.shape[-1]
    mid = width // 2
    n_modes = modes.shape[0]
    here = [lax.axis_index(name) for name in AXES]
    lower = [h > 0 for h in here]
    upper = [h < n - 1 for h, n in zip(here, sizes, strict=True)]
    upper_flag = [jnp.where(u, 1, 0) for u in upper]

    def has_upper(axis):
        x, y, z = upper_flag
        return (x * ((1 - axis) * (2 - axis) // 2) + y * (axis * (2 - axis)) + z * (axis * (axis - 1) // 2)) > 0

    def columns(which, array, scratch, face):
        return pltpu.make_async_copy(
            array.at[:, pl.ds(face * width, width)], scratch.at[face], col_sem.at[which, face]
        )

    def face_block(face):
        return pltpu.make_async_copy(faces_in.at[face], faces.at[face], face_sem.at[face])

    small = [
        pltpu.make_async_copy(source, target, small_sem.at[k])
        for k, (source, target) in enumerate(
            ((mii_in, mii), (modes_in, modes), (mfaces_in, mfaces), (dof_in, dof))
        )
    ]
    for face in (0, 2, 4):
        columns(0, cons_in, cons, face).start()
        columns(1, stiff_in, stiff, face).start()
        face_block(face).start()
    for copy in small:
        copy.start()
    for face in (0, 2, 4):
        columns(2, mass_in, mass, face).start()
    for face in (1, 3, 5):
        columns(0, cons_in, cons, face).start()
        columns(1, stiff_in, stiff, face).start()
        columns(2, mass_in, mass, face).start()
        face_block(face).start()

    barrier = pltpu.get_barrier_semaphore()
    for axis in range(3):

        @pl.when(upper[axis])
        def _(axis=axis):
            pl.semaphore_signal(
                barrier, inc=1, device_id={AXES[axis]: here[axis] + 1}, device_id_type=MESH
            )

    def remote(axis, name, source, target, sems, index):
        return pltpu.make_async_remote_copy(
            src_ref=source,
            dst_ref=target,
            send_sem=sems.at[(0, *index)],
            recv_sem=sems.at[(1, *index)],
            device_id={name: here[AXES.index(name)] - 1},
            device_id_type=MESH,
        )

    def stiff_copy(axis, name="gx"):
        return remote(axis, name, stiff_send.at[axis], stiff_recv.at[axis], stiff_sems, (axis,))

    def mass_copy(axis, name="gx"):
        return remote(axis, name, mass_send.at[axis], mass_recv.at[axis], mass_sems, (axis,))

    def diag_copy(axis, name="gx"):
        return remote(axis, name, diag_send.at[axis], diag_recv.at[axis], diag_sems, (axis,))

    def coup_copy(axis, part, name="gx"):
        rows = pl.ds(*parts[part])
        return remote(
            axis, name, coup_send.at[axis, rows], coup_recv.at[axis, rows], coup_sems, (axis, part)
        )

    for axis in range(3):
        face = 2 * axis
        columns(0, cons_in, cons, face).wait()
        columns(1, stiff_in, stiff, face).wait()
        face_block(face).wait()
        stiff_send[axis] = (turned(stiff[face], cons[face]) + faces[face].astype(F32)).astype(BF16)
        if axis == 0:
            peers = sum(jnp.where(low, 1, 0) for low in lower)

            @pl.when(peers > 0)
            def _():
                pl.semaphore_wait(barrier, peers)

        @pl.when(lower[axis])
        def _(axis=axis):
            stiff_copy(axis, AXES[axis]).start()

    for copy in small:
        copy.wait()
    dcol[...] = column_of(mii[...])
    for face in range(6):
        lump[face] = mfaces[pl.ds(face, 1), :].astype(F32)

    def loaded(face):
        scale = jnp.tile(dcol[...], (1, width // 128))
        load[face] = (mass[face].astype(F32) + scale * cons[face].astype(F32)).astype(BF16)

    row = lax.broadcasted_iota(jnp.int32, (mid, mid), 0)
    column = lax.broadcasted_iota(jnp.int32, (mid, mid), 1)
    left, right = pl.ds(0, mid), pl.ds(mid, mid)
    for axis in range(3):
        face = 2 * axis
        columns(2, mass_in, mass, face).wait()
        loaded(face)

        def block(rows, cols, face=face):
            return turned(cons[face, :, rows], load[face, :, cols]) + turned(
                mass[face, :, rows], cons[face, :, cols]
            )

        lumped = lump[face]
        high_block = block(right, right) + jnp.where(row == column, lumped[:, mid:], 0.0)
        diagonal = jnp.sum(jnp.where(row == column, high_block, 0.0), axis=0, keepdims=True)
        diag_send[axis] = jnp.broadcast_to(diagonal, diag_send.shape[1:]).astype(BF16)
        low_block = block(left, left) + jnp.where(row == column, lumped[:, :mid], 0.0)
        mass_send[axis, :, right] = jnp.where(row <= column, low_block, high_block).astype(BF16)
        mass_send[axis, :, left] = block(left, right).astype(BF16)

        @pl.when(lower[axis])
        def _(axis=axis):
            diag_copy(axis, AXES[axis]).start()
            mass_copy(axis, AXES[axis]).start()

    for axis in range(3):
        coup_send[axis, pl.ds(coup_send.shape[1] - 8, 8), :] = jnp.zeros((8, width), BF16)
        coup_send[axis, pl.ds(0, n_modes), :] = times(modes[...], load[2 * axis]).astype(BF16)

        @pl.when(lower[axis])
        def _(axis=axis):
            for part in range(len(parts)):
                coup_copy(axis, part, AXES[axis]).start()

    for axis in range(3):

        @pl.when(jnp.logical_not(upper[axis]))
        def _(axis=axis):
            stiff_recv[axis] = jnp.zeros(stiff_recv.shape[1:], BF16)
            mass_recv[axis] = jnp.zeros(mass_recv.shape[1:], BF16)
            diag_recv[axis] = jnp.zeros(diag_recv.shape[1:], BF16)
            coup_recv[axis] = jnp.zeros(coup_recv.shape[1:], BF16)

    for face in (1, 3, 5):
        columns(0, cons_in, cons, face).wait()
        columns(1, stiff_in, stiff, face).wait()
        columns(2, mass_in, mass, face).wait()
        face_block(face).wait()

    def own(axis, carry):
        face = 2 * axis + 1
        loaded(face)
        stiff_out[axis] = (turned(stiff[face], cons[face]) + faces[face].astype(F32)).astype(BF16)
        wide_row = lax.broadcasted_iota(jnp.int32, (width, width), 0)
        wide_column = lax.broadcasted_iota(jnp.int32, (width, width), 1)
        lumped = lump[face]
        mass_out[axis] = (
            turned(cons[face], load[face])
            + turned(mass[face], cons[face])
            + jnp.where(wide_row == wide_column, lumped, 0.0)
        ).astype(BF16)
        coup_out[axis, pl.ds(0, n_modes), :] = times(modes[...], load[face]).astype(BF16)
        mapping = dof[axis]
        select[axis] = jnp.where(mapping == wide_row, 1.0, 0.0).astype(BF16)
        spread = jnp.tile(column_of(mapping.astype(F32)), (1, width // 128)).astype(jnp.int32)
        select_t[axis] = jnp.where(spread == wide_column, 1.0, 0.0).astype(BF16)
        return carry

    lax.fori_loop(0, 3, own, 0)

    def reorder(axis, source, out):
        half[...] = times(source, select[axis]).astype(BF16)
        out[axis] = (out[axis].astype(F32) + times(select_t[axis], half[...])).astype(BF16)

    def take_stiff(step, carry):
        axis = lax.rem(step + 2, 3)

        @pl.when(has_upper(axis))
        def _():
            stiff_copy(axis).wait_recv()

        reorder(axis, stiff_recv[axis], stiff_out)
        return carry

    lax.fori_loop(0, 3, take_stiff, 0)

    def take_mass(step, carry):
        axis = lax.rem(step + 2, 3)

        @pl.when(has_upper(axis))
        def _():
            diag_copy(axis).wait_recv()
            mass_copy(axis).wait_recv()

        packed = mass_recv[axis, :, right].astype(F32)
        flipped = packed.T
        across = mass_recv[axis, :, left]
        diagonal = diag_recv[axis].astype(F32)[0:1, :]
        full[left, left] = jnp.where(row <= column, packed, flipped).astype(BF16)
        full[right, right] = jnp.where(
            row > column, packed, jnp.where(row < column, flipped, diagonal)
        ).astype(BF16)
        full[left, right] = across
        full[right, left] = across.astype(F32).T.astype(BF16)
        reorder(axis, full[...], mass_out)
        return carry

    lax.fori_loop(0, 3, take_mass, 0)

    for part, (start, size) in enumerate(parts):

        def take_coup(step, carry, part=part, start=start, size=size):
            axis = lax.rem(step + 2, 3)

            @pl.when(has_upper(axis))
            def _():
                coup_copy(axis, part).wait_recv()

            kept = min(size, n_modes - start)
            moved = times(coup_recv[axis, pl.ds(start, size), :], select[axis]).astype(BF16)
            coup_out[axis, pl.ds(n_modes + start, kept), :] = moved[:kept]
            return carry

        lax.fori_loop(0, 3, take_coup, 0)

    for axis in range(3):

        @pl.when(lower[axis])
        def _(axis=axis):
            stiff_copy(axis).wait_send()
            diag_copy(axis).wait_send()
            mass_copy(axis).wait_send()
            for part in range(len(parts)):
                coup_copy(axis, part).wait_send()


def write_out(stiff_in, mass_in, coup_in, stiff_out, mass_out, coup_out, sems):
    copies = [
        pltpu.make_async_copy(source.at[axis], target.at[axis], sems.at[k, axis])
        for k, (source, target) in enumerate(
            ((stiff_in, stiff_out), (mass_in, mass_out), (coup_in, coup_out))
        )
        for axis in range(3)
    ]
    for copy in copies:
        copy.start()
    for copy in copies:
        copy.wait()


def local(sizes, constraint, stiff_ib, mass_ib, mass_ii, modes, stiff_faces, mass_faces, dof_map):
    depth = constraint.shape[-2]
    width = stiff_faces.shape[-1]
    n_modes = modes.shape[-2]
    mid = width // 2
    tall = -(-n_modes // 8) * 8
    quarter = -(-tall // 32) * 8
    parts = [(start, min(quarter, tall - start)) for start in range(0, tall, quarter)]
    shapes = ((3, width, width), (3, width, width), (3, 2 * n_modes, width))
    hbm = pl.BlockSpec(memory_space=pltpu.HBM)
    vmem = pl.BlockSpec(memory_space=pltpu.VMEM)
    dma = pltpu.SemaphoreType.DMA
    blocks = pl.pallas_call(
        functools.partial(exchange, sizes, parts),
        out_shape=[pltpu.VMEM(shape, BF16) for shape in shapes],
        in_specs=[hbm] * 8,
        out_specs=[vmem] * 3,
        scratch_shapes=[
            pltpu.VMEM((6, depth, width), BF16),
            pltpu.VMEM((6, depth, width), BF16),
            pltpu.VMEM((6, depth, width), BF16),
            pltpu.VMEM((1, depth), F32),
            pltpu.VMEM((n_modes, depth), BF16),
            pltpu.VMEM((6, width, width), BF16),
            pltpu.VMEM((6, width), BF16),
            pltpu.VMEM((3, 1, width), jnp.int32),
            pltpu.VMEM((6, 1, width), F32),
            pltpu.VMEM((6, depth, width), BF16),
            pltpu.VMEM((3, width, width), BF16),
            pltpu.VMEM((3, width, width), BF16),
            pltpu.VMEM((depth, 128), F32),
            pltpu.VMEM((width, width), BF16),
            pltpu.VMEM((width, width), BF16),
            pltpu.VMEM((3, width, width), BF16),
            pltpu.VMEM((3, mid, width), BF16),
            pltpu.VMEM((3, 16, mid), BF16),
            pltpu.VMEM((3, tall, width), BF16),
            pltpu.VMEM((3, width, width), BF16),
            pltpu.VMEM((3, mid, width), BF16),
            pltpu.VMEM((3, 16, mid), BF16),
            pltpu.VMEM((3, tall, width), BF16),
            dma((3, 6)),
            dma((6,)),
            dma((4,)),
            dma((2, 3)),
            dma((2, 3)),
            dma((2, 3)),
            dma((2, 3, len(parts))),
        ],
        compiler_params=pltpu.CompilerParams(
            collective_id=0, has_side_effects=True, vmem_limit_bytes=48 * 2**20
        ),
        name="exchange",
    )(*(pltpu.with_memory_space_constraint(a, pltpu.HBM) for a in (
        constraint[0, 0, 0],
        stiff_ib[0, 0, 0],
        mass_ib[0, 0, 0],
        mass_ii.reshape(1, depth),
        modes[0, 0, 0],
        stiff_faces[0, 0, 0],
        mass_faces[0, 0, 0],
        dof_map[0, 0, 0][:, None],
    )))
    outs = pl.pallas_call(
        write_out,
        out_shape=[jax.ShapeDtypeStruct(shape, BF16) for shape in shapes],
        in_specs=[vmem] * 3,
        out_specs=[hbm] * 3,
        scratch_shapes=[dma((3, 3))],
        compiler_params=pltpu.CompilerParams(vmem_limit_bytes=2**20),
        name="write_out",
    )(*(pltpu.with_memory_space_constraint(b, pltpu.VMEM) for b in blocks))
    return tuple(out[None, None, None] for out in outs)


def solution(mesh):
    sizes = tuple(mesh.shape[name] for name in AXES)
    grid = P("gx", "gy", "gz")
    return jax.shard_map(
        functools.partial(local, sizes),
        mesh=mesh,
        in_specs=(grid,) * 8,
        out_specs=(grid,) * 3,
        check_vma=False,
    )
```
